32 devices in a mesh: rows: 8 (over y, x, core), cols: 4 (over z).
Axes of the slice: x: 2, y: 2, z: 4, core: 2. Of those that a mesh axis runs over, the one named last changes fastest.
Arguments:
- one_query: float32 [8192, 8192], P('rows', 'cols'), may hold values from -0.09375 to 0.09375
- other_query: float32 [8192, 8192], P('rows', 'cols'), may hold values from -0.0625 to 0.0625
- one_key: float32 [8192, 512], P('rows', 'cols'), may hold values from -0.09375 to 0.09375
- other_key: float32 [8192, 512], P('rows', 'cols'), may hold values from -0.0625 to 0.0625
- one_value: float32 [8192, 512], P('rows', 'cols'), may hold values from -0.09375 to 0.09375
- other_value: float32 [8192, 512], P('rows', 'cols'), may hold values from -0.0625 to 0.0625
- mix_share: float32 [8192], P('rows'), may hold values from 0.2 to 0.8
- norm_gain: float32 [8192], P('rows'), may hold values from 0.25 to 1.75
Outputs:
- serve_query: bfloat16 [8192, 8192], P(None, 'cols')
- serve_key: bfloat16 [8192, 512], P(None, 'cols')
- serve_value: bfloat16 [8192, 512], P(None, 'cols')
- scale_query: float32 [8192], P('cols')
- scale_key: float32 [512], P('cols')
- scale_value: float32 [512], P('cols')
The draws below stay inside these ranges and needn't reach their ends.
All inputs are finite; a program needn't handle non-finite values. Where the reference program divides by a largest or mean magnitude, that divisor is 1e-20 or more.
Results may differ from the reference program's by a relative error of at most 0.001.
Values may be sent and summed in bfloat16 or wider, within the bound.
A program may use at most 192 MiB of HBM per device.

```python
import jax
import jax.numpy as jnp

D_MODEL = 8192
Q_DIM = 8192
KV_DIM = 512


def strengthened(drawn, stream_key, source, target, parts, factor):
    owner, partner = [(jnp.arange(drawn.shape[dim]) // (drawn.shape[dim] // parts)).reshape([-1 if axis == dim else 1 for axis in range(drawn.ndim)]) for dim in (source, target)]
    chosen = jax.random.permutation(stream_key, parts)[partner]
    strong = (owner == chosen) | (owner == (partner + parts // 2) % parts)
    return jnp.where(strong, factor * drawn, drawn)


def block_levels(own_key, extent, cuts, low, high):
    level, own = 1.0, jax.random.fold_in(own_key, 6)
    for axis_at, parts in cuts:
        steps = jnp.exp(jax.random.uniform(jax.random.fold_in(own, axis_at), (parts,), jnp.float32, low / len(cuts), high / len(cuts)))
        level = level * jnp.repeat(steps, extent[axis_at] // parts).reshape([-1 if axis == axis_at else 1 for axis in range(len(extent))])
    return level


def gaussian(own_key, extent, width, reach, shards=(), dtype=jnp.bfloat16):
    drawn = width * jax.random.normal(own_key, extent, jnp.float32)
    if shards:
        drawn = drawn * block_levels(own_key, extent, shards, -0.22, 0.18)
    return jnp.clip(drawn, -reach, reach).astype(dtype)


def gaussian_with(own_key, dims, deviation, reach, cuts, heavy, dtype=jnp.bfloat16):
    drawn = deviation * jax.random.normal(own_key, dims, jnp.float32)
    if cuts:
        drawn = drawn * block_levels(own_key, dims, cuts, -0.22, 0.18)
    return jnp.clip(strengthened(drawn, jax.random.fold_in(own_key, 3), *heavy), -reach, reach).astype(dtype)


def setup_inputs(seed: int = 0) -> dict:
    streams_of = jax.random.split(jax.random.key(seed), 9)
    one_query = gaussian_with(streams_of[0], (D_MODEL, Q_DIM), D_MODEL ** -0.5, 0.09375, ((0, 8), (1, 4)), (0, 1, 8, 2.0), jnp.float32)
    other_query = gaussian(streams_of[1], (D_MODEL, Q_DIM), D_MODEL ** -0.5, 0.0625, ((0, 8), (1, 4)), jnp.float32)
    one_key = gaussian_with(streams_of[2], (D_MODEL, KV_DIM), D_MODEL ** -0.5, 0.09375, ((0, 8), (1, 4)), (0, 1, 8, 2.0), jnp.float32)
    other_key = gaussian(streams_of[3], (D_MODEL, KV_DIM), D_MODEL ** -0.5, 0.0625, ((0, 8), (1, 4)), jnp.float32)
    one_value = gaussian_with(streams_of[4], (D_MODEL, KV_DIM), D_MODEL ** -0.5, 0.09375, ((0, 8), (1, 4)), (0, 1, 8, 2.0), jnp.float32)
    other_value = gaussian(streams_of[5], (D_MODEL, KV_DIM), D_MODEL ** -0.5, 0.0625, ((0, 8), (1, 4)), jnp.float32)
    mix_share = jnp.clip(0.2 + 0.6 * jax.random.uniform(streams_of[6], (D_MODEL,), jnp.float32) ** block_levels(streams_of[6], (D_MODEL,), ((0, 8),), -0.2, 0.2), 0.2, 0.8)
    norm_gain = jnp.clip(1.0 + 0.15 * jax.random.normal(streams_of[7], (D_MODEL,), jnp.float32), 0.25, 1.75)
    return dict(one_query=one_query, other_query=other_query, one_key=one_key, other_key=other_key, one_value=one_value, other_value=other_value, mix_share=mix_share, norm_gain=norm_gain)


def reference(one_query, other_query, one_key, other_key, one_value, other_value, mix_share, norm_gain):
    fresh_query = mix_share[:, None] * one_query + (1.0 - mix_share[:, None]) * other_query
    fresh_key = mix_share[:, None] * one_key + (1.0 - mix_share[:, None]) * other_key
    fresh_value = mix_share[:, None] * one_value + (1.0 - mix_share[:, None]) * other_value
    fresh_gained_query = fresh_query * norm_gain[:, None]
    fresh_gained_key = fresh_key * norm_gain[:, None]
    fresh_gained_value = fresh_value * norm_gain[:, None]
    scale_query = jnp.sum(jnp.abs(fresh_gained_query), axis=0) / D_MODEL
    serve_query = (fresh_gained_query / scale_query).astype(jnp.bfloat16)
    scale_key = jnp.sum(jnp.abs(fresh_gained_key), axis=0) / D_MODEL
    serve_key = (fresh_gained_key / scale_key).astype(jnp.bfloat16)
    scale_value = jnp.sum(jnp.abs(fresh_gained_value), axis=0) / D_MODEL
    serve_value = (fresh_gained_value / scale_value).astype(jnp.bfloat16)
    return serve_query, serve_key, serve_value, scale_query, scale_key, scale_value
```

```python
import functools
import math

import jax
import jax.numpy as jnp
from jax import lax
from jax.experimental import pallas as pl
from jax.experimental.pallas import tpu as pltpu
from jax.sharding import PartitionSpec as P

MESH = pl.DeviceIdType.MESH
CHUNK = 256
STEP_ROWS = 64


def ring_of(chips):
    side = math.isqrt(chips)
    if side * side != chips or side % 2 or side < 2:
        return list(range(chips))
    cycle = [y * side for y in range(side)]
    for k in range(side):
        y = side - 1 - k
        xs = range(1, side) if k % 2 == 0 else range(side - 1, 0, -1)
        cycle += [y * side + x for x in xs]
    return cycle


def pick(table, index):
    out = jnp.int32(table[0])
    for at in range(1, len(table)):
        out = jnp.where(index == at, jnp.int32(table[at]), out)
    return out


def kernel(
    ranks, d_model, plan,
    share_ref, rest_ref, oq, tq, ok, tk, ov, tv,
    sq, sk, sv, cq, ck, cv,
    one_wide, other_wide, narrow_wide, mine_wide, sums_wide,
    one_slim, other_slim, narrow_slim, mine_slim, sums_slim,
    in_sem, stat_send, stat_recv, own_sem, ring_send, ring_recv, twin_send, twin_recv,
):
    me = lax.axis_index("rows")
    chips = ranks // 2
    chip, core = me // 2, me % 2
    cycle = ring_of(chips)
    place = [cycle.index(c) for c in range(chips)]
    spot = pick(place, chip)
    ahead = pick([cycle[(place[c] + 1) % chips] for c in range(chips)], chip)
    behind = pick([cycle[(place[c] - 1) % chips] for c in range(chips)], chip)
    next_dev = (ahead * 2 + core, behind * 2 + core)
    twin = chip * 2 + 1 - core
    rows = oq.shape[0]
    half = rows // 2
    steps = chips // 2
    firsts, others = (oq, ok, ov), (tq, tk, tv)
    outs, scales = (sq, sk, sv), (cq, ck, cv)

    one, other, narrow, mine, sums = {}, {}, {}, {}, {}
    for j, (which, slot, col, width) in enumerate(plan):
        slim = which > 0
        one[j] = (one_slim if slim else one_wide).at[slot]
        other[j] = (other_slim if slim else other_wide).at[slot]
        narrow[j] = (narrow_slim if slim else narrow_wide).at[slot]
        mine[j] = (mine_slim if slim else mine_wide).at[slot]
        for shift in range(1, ranks):
            sums[shift, j] = (sums_slim if slim else sums_wide).at[shift, slot]

    def window(ref, j, first, count):
        which, slot, col, width = plan[j]
        if which > 0:
            return ref.at[pl.ds(first, count)]
        return ref.at[pl.ds(first, count), pl.ds(col, width)]

    def origin(way, step):
        at = lax.rem(spot - step + chips, chips) if way == 0 else lax.rem(spot + step, chips)
        return pick(cycle, at) * 2 + core

    def span(way, step):
        if chips % 2 == 0 and step == steps:
            return way * half, half
        return 0, rows

    loads = []
    for j, (which, slot, col, width) in enumerate(plan):
        pair = []
        for k, (source, held) in enumerate(((firsts, one), (others, other))):
            copy = pltpu.make_async_copy(
                window(source[which], j, 0, rows),
                held[j],
                in_sem.at[k, j],
            )
            copy.start()
            pair.append(copy)
        loads.append(pair)

    barrier = pltpu.get_barrier_semaphore()
    for shift in range(1, ranks):
        pl.semaphore_signal(
            barrier, inc=1, device_id={"rows": lax.rem(me + shift, ranks)}, device_id_type=MESH
        )

    stat_copies = {}
    pending = []

    def tiles(width):
        return [(c, min(128, width - c)) for c in range(0, width, 128)]

    def measure(j):
        which, slot, col, width = plan[j]
        loads[j][0].wait()
        loads[j][1].wait()
        cuts = tiles(width)

        def body(i, accs):
            r = pl.ds(pl.multiple_of(i * STEP_ROWS, STEP_ROWS), STEP_ROWS)
            new = []
            for (c, w), acc in zip(cuts, accs):
                a, b = share_ref[r, pl.ds(0, w)], rest_ref[r, pl.ds(0, w)]
                f = a * one[j][r, pl.ds(c, w)] + b * other[j][r, pl.ds(c, w)]
                one[j][r, pl.ds(c, w)] = f
                new.append(acc + jnp.sum(jnp.abs(f).reshape(STEP_ROWS // 8, 8, w), axis=0))
            return tuple(new)

        accs = lax.fori_loop(
            0, rows // STEP_ROWS, body, tuple(jnp.zeros((8, w), jnp.float32) for _, w in cuts)
        )
        for (c, w), acc in zip(cuts, accs):
            mine[j][:, pl.ds(c, w)] = jnp.sum(acc, axis=0, keepdims=True)

    def share(j):
        if j == 0:
            pl.semaphore_wait(barrier, ranks - 1)
        for shift in range(1, ranks):
            copy = pltpu.make_async_remote_copy(
                src_ref=mine[j],
                dst_ref=sums[shift, j],
                send_sem=stat_send.at[shift, j],
                recv_sem=stat_recv.at[shift, j],
                device_id={"rows": lax.rem(me + shift, ranks)},
                device_id_type=MESH,
            )
            copy.start()
            stat_copies[shift, j] = copy

    def remote(src, dst, send, recv, device):
        copy = pltpu.make_async_remote_copy(
            src_ref=src, dst_ref=dst, send_sem=send, recv_sem=recv,
            device_id={"rows": device}, device_id_type=MESH,
        )
        copy.start()
        return copy

    def block(j, dev, first, count):
        which, slot, col, width = plan[j]
        start = pl.multiple_of(dev * rows + first, half)
        return window(outs[which], j, start, count)

    ring = {}
    twins = {}

    def finish(j):
        which, slot, col, width = plan[j]
        for shift in range(1, ranks):
            stat_copies[shift, j].wait()
        inverses = []
        for c, w in tiles(width):
            total = jnp.zeros((1, w), jnp.float32)
            for owner in range(ranks):
                part = mine[j][:, pl.ds(c, w)]
                for shift in range(1, ranks):
                    sent = sums[shift, j][:, pl.ds(c, w)]
                    part = jnp.where(lax.rem(me - owner + ranks, ranks) == shift, sent, part)
                total = total + part
            scale = total / d_model
            scales[which][:, pl.ds(col + c, w)] = scale
            inverses.append(1.0 / scale)

        def body(i, carry):
            r = pl.ds(pl.multiple_of(i * STEP_ROWS, STEP_ROWS), STEP_ROWS)
            for (c, w), inverse in zip(tiles(width), inverses):
                narrow[j][r, pl.ds(c, w)] = (one[j][r, pl.ds(c, w)] * inverse).astype(jnp.bfloat16)
            return carry

        lax.fori_loop(0, rows // STEP_ROWS, body, 0)

    def send(j):
        which, slot, col, width = plan[j]
        for way in range(2):
            if steps:
                first, count = span(way, 1)
                ring[way, 1, j] = remote(
                    narrow[j].at[pl.ds(first, count)],
                    block(j, me, first, count),
                    ring_send.at[way, 0, j], ring_recv.at[way, 0, j], next_dev[way],
                )
        twins[0, 0, j] = remote(
            narrow[j], block(j, me, 0, rows),
            twin_send.at[0, 0, j], twin_recv.at[0, 0, j], twin,
        )
        copy = pltpu.make_async_copy(
            narrow[j], block(j, me, 0, rows), own_sem.at[j]
        )
        copy.start()
        pending.append(copy)

    count = len(plan)
    measure(0)
    share(0)
    for j in range(count):
        if j + 1 < count:
            measure(j + 1)
            share(j + 1)
        finish(j)
        send(j)

    for step in range(1, steps + 1):
        for j in range(count):
            for way in range(2):
                ring[way, step, j].wait_recv()
                dev = origin(way, step)
                if step < steps:
                    first, n = span(way, step + 1)
                    piece = block(j, dev, first, n)
                    ring[way, step + 1, j] = remote(
                        piece, piece,
                        ring_send.at[way, step, j], ring_recv.at[way, step, j], next_dev[way],
                    )
                first, n = span(way, step)
                piece = block(j, dev, first, n)
                twins[way, step, j] = remote(
                    piece, piece,
                    twin_send.at[way, step, j], twin_recv.at[way, step, j], twin,
                )
    for copy in pending:
        copy.wait()
    for copy in ring.values():
        copy.wait_send()
    for copy in twins.values():
        copy.wait()


def local(ranks, d_model, one_query, other_query, one_key, other_key, one_value, other_value, mix_share, norm_gain):
    rows, q_cols = one_query.shape
    kv_cols = one_key.shape[1]
    width = min(CHUNK, q_cols)
    plan = [(0, col // width, col, width) for col in range(0, q_cols, width)]
    plan += [(1, 0, 0, kv_cols), (2, 1, 0, kv_cols)]
    scratch = []
    for slots, wide in ((q_cols // width, width), (2, kv_cols)):
        scratch += [
            pltpu.VMEM((slots, rows, wide), jnp.float32),
            pltpu.VMEM((slots, rows, wide), jnp.float32),
            pltpu.VMEM((slots, rows, wide), jnp.bfloat16),
            pltpu.VMEM((slots, 1, wide), jnp.float32),
            pltpu.VMEM((ranks, slots, 1, wide), jnp.float32),
        ]
    count = len(plan)
    steps = ranks // 4
    share = jnp.broadcast_to((norm_gain * mix_share)[:, None], (rows, 128))
    rest = jnp.broadcast_to((norm_gain * (1.0 - mix_share))[:, None], (rows, 128))
    whole = ranks * rows
    vmem = pl.BlockSpec(memory_space=pltpu.VMEM)
    hbm = pl.BlockSpec(memory_space=pl.ANY)
    dma = pltpu.SemaphoreType.DMA
    sq, sk, sv, cq, ck, cv = pl.pallas_call(
        functools.partial(kernel, ranks, d_model, plan),
        out_shape=(
            jax.ShapeDtypeStruct((whole, q_cols), jnp.bfloat16),
            jax.ShapeDtypeStruct((whole, kv_cols), jnp.bfloat16),
            jax.ShapeDtypeStruct((whole, kv_cols), jnp.bfloat16),
            jax.ShapeDtypeStruct((1, q_cols), jnp.float32),
            jax.ShapeDtypeStruct((1, kv_cols), jnp.float32),
            jax.ShapeDtypeStruct((1, kv_cols), jnp.float32),
        ),
        in_specs=[vmem, vmem] + [hbm] * 6,
        out_specs=(hbm, hbm, hbm, vmem, vmem, vmem),
        scratch_shapes=scratch
        + [
            dma((2, count)),
            dma((ranks, count)),
            dma((ranks, count)),
            dma((count,)),
            dma((2, max(steps, 1), count)),
            dma((2, max(steps, 1), count)),
            dma((2, steps + 1, count)),
            dma((2, steps + 1, count)),
        ],
        compiler_params=pltpu.CompilerParams(
            collective_id=0, has_side_effects=True, vmem_limit_bytes=50 * 1024 * 1024
        ),
    )(share, rest, one_query, other_query, one_key, other_key, one_value, other_value)
    return sq, sk, sv, cq[0], ck[0], cv[0]


def solution(mesh):
    def body(one_query, *rest):
        ranks = mesh.shape["rows"]
        return local(ranks, ranks * one_query.shape[0], one_query, *rest)

    return jax.shard_map(
        body,
        mesh=mesh,
        in_specs=(P("rows", "cols"),) * 6 + (P("rows"),) * 2,
        out_specs=(P(None, "cols"),) * 3 + (P("cols"),) * 3,
        check_vma=False,
    )
```
